32 devices in a mesh: groups: 2 (over x), seq: 16 (over z, y, core).
Axes of the slice: x: 2, y: 2, z: 4, core: 2. Of those that a mesh axis runs over, the one named last changes fastest.
Arguments:
- queries: bfloat16 [8192, 4096], P(('groups', 'seq')), parts along dimension 0, may hold values from -13 to 13
- keys: bfloat16 [8192, 512], P(('groups', 'seq')), parts along dimension 0, may hold values from -13 to 13
- values: bfloat16 [8192, 512], P(('groups', 'seq')), parts along dimension 0, may hold values from -6 to 6
- segment_ids: int32 [8192], P(('groups', 'seq')), parts along dimension 0, may hold values from 0 to 8, as said below
Outputs:
- attended: bfloat16 [8192, 4096], P(('groups', 'seq')), parts along dimension 0
- rotated_keys: bfloat16 [8192, 512], P(('groups', 'seq')), parts along dimension 0
The draws below stay inside these ranges and needn't reach their ends.
There are 2 independent parts, one for each index of `groups`. The reference program is written for one: setup_inputs(seed, part) draws one part's arguments, and reference() takes and returns one part's arrays. A program takes and returns all parts, laid end to end along the dimension named above; each array names one. Nothing has to cross between parts.
Inputs may be any that keep to these rules, and one draw needn't show every extreme that they name: `segment_ids`: never falling along the packed stream, starting at 0 and rising by one at each new rollout; each rollout covers 1 to 1792 tokens and one covers exactly 1792.
All inputs are finite; a program needn't handle non-finite values.
Results may differ from the reference program's by a relative error of at most 0.0054.
Values may be sent and summed in bfloat16 or wider, within the bound.
A program may use at most 192 MiB of HBM per device.

```python
import jax
import jax.numpy as jnp
from jax import lax

HQ = 32
HK = 4
HD = 128
SPAN = 7
TOK_DEV = 256
TOKENS = 4096
N_SEQ = 16


def base_draw(own_key, width):
    return jnp.clip(jax.random.normal(own_key, (TOKENS, width), jnp.float32), -6.0, 6.0)


def draw_queries(key, part):
    drawn = base_draw(jax.random.fold_in(key, 21), HQ * HD)
    return drawn.astype(jnp.bfloat16)


def draw_keys(key, part):
    drawn = base_draw(jax.random.fold_in(key, 22), HK * HD)
    return drawn.astype(jnp.bfloat16)


def draw_segment_ids(key, part):
    quarter = TOK_DEV // 4
    offset_key = jax.random.fold_in(key, 31)
    lead_offset = jax.random.randint(jax.random.fold_in(offset_key, 1), (), 1, quarter)
    first_cut = (N_SEQ // 2 - 1) * TOK_DEV + jax.random.randint(jax.random.fold_in(offset_key, 2), (), 1, TOK_DEV)
    second_cut = N_SEQ // 2 * TOK_DEV + jax.random.randint(jax.random.fold_in(offset_key, 3), (), 1, TOK_DEV)
    third_cut = (N_SEQ // 2 + 1) * TOK_DEV + jax.random.randint(jax.random.fold_in(offset_key, 4), (), 1, TOK_DEV)
    window_count = N_SEQ // 2
    window_number = jnp.arange(window_count, dtype=jnp.int32)
    window_shift = jax.random.randint(jax.random.fold_in(offset_key, 5), (window_count,), 0, TOK_DEV)
    window_place = window_number * (2 * TOK_DEV) + window_shift
    window_used = (window_number >= 4) & (window_number != N_SEQ // 4 - 1) & (window_number != N_SEQ // 4)
    window_place = jnp.where(window_used, window_place, 0)
    marks = jnp.zeros((TOKENS,), jnp.int32)
    marks = marks.at[window_place].max(window_used.astype(jnp.int32))
    marks = marks.at[0].set(1)
    marks = marks.at[lead_offset].set(1)
    marks = marks.at[lead_offset + SPAN * TOK_DEV].set(1)
    marks = marks.at[first_cut].set(1)
    marks = marks.at[second_cut].set(1)
    marks = marks.at[third_cut].set(1)
    return (jnp.cumsum(marks) - 1).astype(jnp.int32)


def shard_levels(key, shape, shards, smallest, top_value):
    def one(axis_at, blocks):
        heights = jax.random.uniform(jax.random.fold_in(jax.random.fold_in(key, 6), axis_at), (blocks,), jnp.float32, smallest / len(shards), top_value / len(shards))
        return jnp.repeat(jnp.exp(heights), shape[axis_at] // blocks).reshape((-1,) + (1,) * (len(shape) - axis_at - 1))

    loudness = one(*shards[0])
    for cut in shards[1:]:
        loudness = loudness * one(*cut)
    return loudness


def gaussian(rng, shape, deviation, most, split=(), kind=jnp.bfloat16):
    entries = deviation * jax.random.normal(rng, shape, jnp.float32)
    if split:
        entries = entries * shard_levels(rng, shape, split, -0.22, 0.18)
    return jnp.clip(entries, -most, most).astype(kind)


def setup_inputs(seed: int = 0, part: int = 0) -> dict:
    splits = jax.random.split(jax.random.key(seed), 5)
    part_splits = jax.random.split(jax.random.fold_in(splits[4], part), 5)
    queries = draw_queries(jax.random.fold_in(jax.random.fold_in(splits[4], part), 71), part)
    keys = draw_keys(jax.random.fold_in(jax.random.fold_in(splits[4], part), 71), part)
    values = gaussian(part_splits[2], (TOKENS, HK * HD), 1.0, 6.0, ((0, 16),))
    segment_ids = draw_segment_ids(jax.random.fold_in(jax.random.fold_in(splits[4], part), 71), part)
    return dict(queries=queries, keys=keys, values=values, segment_ids=segment_ids)


ROPE_BASE = 1000000.0
MASKED_SCORE = -1.0e30


def rollout_starts(segment_ids):
    token_index = jnp.arange(segment_ids.shape[0], dtype=jnp.int32)
    boundary = jnp.concatenate([jnp.ones((1,), dtype=jnp.bool_), segment_ids[1:] != segment_ids[:-1]])
    return lax.cummax(jnp.where(boundary, token_index, -1), axis=0)


def rotate_heads(matrix, positions, head_count):
    row_count = matrix.shape[0]
    half_dim = HD // 2
    inverse_freq = ROPE_BASE ** (-(jnp.arange(half_dim, dtype=jnp.float32) * (2.0 / HD)))
    angles = positions.astype(jnp.float32)[:, None] * inverse_freq[None, :]
    cosine = jnp.cos(angles)[:, None, :]
    sine = jnp.sin(angles)[:, None, :]
    split_heads = matrix.astype(jnp.float32).reshape(row_count, head_count, HD)
    lower_half = split_heads[..., :half_dim]
    upper_half = split_heads[..., half_dim:]
    turned = jnp.concatenate([lower_half * cosine - upper_half * sine, upper_half * cosine + lower_half * sine], axis=-1)
    return turned.reshape(row_count, head_count * HD).astype(jnp.bfloat16)


def reference(queries, keys, values, segment_ids):
    token_count = queries.shape[0]
    starts = rollout_starts(segment_ids)
    positions = jnp.arange(token_count, dtype=jnp.int32) - starts
    turned_queries = rotate_heads(queries, positions, HQ)
    rotated_keys = rotate_heads(keys, positions, HK)
    reach_rows = SPAN * TOK_DEV
    window_rows = (SPAN + 1) * TOK_DEV
    group_size = HQ // HK
    padded_keys = jnp.concatenate([jnp.zeros((reach_rows, HK * HD), jnp.bfloat16), rotated_keys], axis=0)
    padded_values = jnp.concatenate([jnp.zeros((reach_rows, HK * HD), jnp.bfloat16), values], axis=0)

    def one_block(block_number):
        block_first = (block_number * TOK_DEV).astype(jnp.int32)
        query_block = lax.dynamic_slice_in_dim(turned_queries, block_first, TOK_DEV, 0).astype(jnp.float32).reshape(TOK_DEV, HK, group_size, HD)
        key_window = lax.dynamic_slice_in_dim(padded_keys, block_first, window_rows, 0).astype(jnp.float32).reshape(window_rows, HK, HD)
        value_window = lax.dynamic_slice_in_dim(padded_values, block_first, window_rows, 0).astype(jnp.float32).reshape(window_rows, HK, HD)
        query_starts = lax.dynamic_slice_in_dim(starts, block_first, TOK_DEV, 0)
        query_index = block_first + jnp.arange(TOK_DEV, dtype=jnp.int32)
        key_index = block_first - reach_rows + jnp.arange(window_rows, dtype=jnp.int32)
        allowed = (key_index[None, :] >= query_starts[:, None]) & (key_index[None, :] <= query_index[:, None])
        scores = jnp.einsum("thgd,shd->thgs", query_block, key_window) * (HD ** -0.5)
        scores = jnp.where(allowed[:, None, None, :], scores, MASKED_SCORE)
        row_top = jnp.max(scores, axis=-1, keepdims=True)
        weights = jnp.exp(scores - row_top)
        totals = jnp.sum(weights, axis=-1, keepdims=True)
        rounded_weights = lax.optimization_barrier(weights.astype(jnp.bfloat16)).astype(jnp.float32)
        mixed = jnp.einsum("thgs,shd->thgd", rounded_weights, value_window) / totals
        return mixed.reshape(TOK_DEV, HQ * HD).astype(jnp.bfloat16)

    attended = lax.map(one_block, jnp.arange(N_SEQ, dtype=jnp.int32))
    return (attended.reshape(token_count, HQ * HD), rotated_keys)
```

```python
from functools import partial

import jax
import jax.numpy as jnp
import numpy as np
from jax import lax
from jax.experimental import pallas as pl
from jax.experimental.pallas import tpu as pltpu
from jax.sharding import PartitionSpec as P

HD = 128
HALF = HD // 2
SPAN = 7
ROPE_BASE = 1000000.0
BIG = 1e30
NO_SEGMENT = -1
ONES_ROWS = 16
STEP = 16
SLOTS = SPAN + 2
LOG2E = 1.4426950408889634


def kernel(
    kv_heads, count, q_hbm, k_hbm, v_hbm, seg_hbm, freq_ref, out_ref, rot_ref,
    kraw, vraw, segs, qraw, qa, qext, krot, kext, vt, ctab, stab, mask, scores_a, scores_b,
    top, acc, local_sems, send_sems, recv_sems, seg_send, seg_recv,
):
    rows = kraw.shape[1]
    heads = qa.shape[0]
    group = heads // kv_heads
    me = lax.axis_index("seq")
    core = lax.rem(me, 2)
    side = lax.rem(me // 2, 2)
    plane = me // 4
    planes = count // 4
    partner = me + 1 - 2 * core
    across = me + 2 - 4 * side
    ahead = me + 4
    behind = me - 4
    has_ahead = plane + 1 < planes
    has_behind = plane >= 1

    barrier = pltpu.get_barrier_semaphore()

    def greet(device):
        pl.semaphore_signal(
            barrier, inc=1, device_id={"seq": device}, device_id_type=pl.DeviceIdType.MESH
        )

    greet(partner)
    greet(across)

    @pl.when(has_ahead)
    def _():
        greet(ahead)

    @pl.when(has_behind)
    def _():
        greet(behind)

    def columns(kv):
        return pl.ds(pl.multiple_of(kv * HD, HD), HD)

    def load(index, src, dst):
        return pltpu.make_async_copy(src, dst, local_sems.at[index])

    seg_load = load(0, seg_hbm, segs.at[0])
    seg_load.start()
    loads = []
    for kv in range(kv_heads):
        at = slice(kv * HD, (kv + 1) * HD)
        loads.append((
            load(1 + 2 * kv, k_hbm.at[:, at], kraw.at[0, :, at]),
            load(2 + 2 * kv, v_hbm.at[:, at], vraw.at[0, :, at]),
        ))
        for one in loads[-1]:
            one.start()
    wide = group * HD
    q_loads = []
    for kv in range(kv_heads):
        at = slice(kv * wide, (kv + 1) * wide)
        q_loads.append(load(1 + 2 * kv_heads + kv, q_hbm.at[:, at], qraw.at[:, at]))
        q_loads[-1].start()

    both = has_ahead & has_behind
    one_side = (has_ahead | has_behind) & jnp.logical_not(both)
    neither = jnp.logical_not(has_ahead | has_behind)
    for extra, condition in ((2, both), (1, one_side), (0, neither)):

        @pl.when(condition)
        def _():
            pl.semaphore_wait(barrier, 2 + extra)

    def piece_copy(kind, half, kv, source, distance, device):
        buffer = (kraw, vraw)[half]
        return pltpu.make_async_remote_copy(
            src_ref=buffer.at[source, :, columns(kv)],
            dst_ref=buffer.at[distance, :, columns(kv)],
            send_sem=send_sems.at[kind, kv, half],
            recv_sem=recv_sems.at[distance, kv, half],
            device_id={"seq": device},
            device_id_type=pl.DeviceIdType.MESH,
        )

    def seg_copy(kind, source, distance, device):
        return pltpu.make_async_remote_copy(
            src_ref=segs.at[source],
            dst_ref=segs.at[distance],
            send_sem=seg_send.at[kind],
            recv_sem=seg_recv.at[distance],
            device_id={"seq": device},
            device_id_type=pl.DeviceIdType.MESH,
        )

    to_partner = 1 - 2 * core
    relays = core == 1
    has_two = (side == 1) | has_behind
    has_six = ((side == 1) & has_behind) | (plane >= 2)
    has_eight = (plane >= 2) & relays
    flows = {
        0: (has_ahead, 0, 4, ahead),
        1: (side == 0, 0, 2, across),
        2: (core == 0, 0, 1, partner),
        3: (has_behind, 4, 6 - 4 * side, across),
        4: (has_behind & has_ahead & relays, 4, 8, ahead),
        5: (has_behind, 4, 4 + to_partner, partner),
        6: (has_two, 2, 2 + to_partner, partner),
        7: (has_eight & (side == 1), 8, 6, across),
        8: (has_eight, 8, 7, partner),
        9: (has_six, 6, 6 + to_partner, partner),
        10: ((side == 0) & (core == 0) & has_behind & has_ahead, 2, 6, ahead),
    }

    def send(kinds, half, kv):
        for kind in kinds:
            condition, source, distance, device = flows[kind]

            @pl.when(condition)
            def _():
                piece_copy(kind, half, kv, source, distance, device).start()

    def send_segs(kinds):
        for kind in kinds:
            condition, source, distance, device = flows[kind]

            @pl.when(condition)
            def _():
                seg_copy(kind, source, distance, device).start()

    def arrive(condition, distance, half, kv):
        @pl.when(condition)
        def _():
            piece_copy(0, half, kv, 0, distance, partner).wait_recv()

    def arrive_segs(condition, distance):
        @pl.when(condition)
        def _():
            seg_copy(0, 0, distance, partner).wait_recv()

    def relay(condition, distance, kinds, kv):
        for half in range(2):
            arrive(condition, distance, half, kv)
            send(kinds, half, kv)

    def relay_segs(condition, distance, kinds):
        arrive_segs(condition, distance)
        send_segs(kinds)

    seg_load.wait()
    send_segs((0, 1, 2))
    for kv in range(kv_heads):
        for half in range(2):
            loads[kv][half].wait()
            send((0, 1, 2), half, kv)

    for distance in range(1, SPAN + 1):

        @pl.when(me < distance)
        def _():
            segs[distance] = jnp.full(segs.shape[1:], NO_SEGMENT, jnp.int32)
            kraw[distance] = jnp.zeros(kraw.shape[1:], jnp.bfloat16)
            vraw[distance] = jnp.zeros(vraw.shape[1:], jnp.bfloat16)

    freq = freq_ref[...]
    lane = lax.broadcasted_iota(jnp.int32, (1, HD), 1)
    sign = jnp.where(lane < HALF, -1.0, 1.0)

    def fan(steps, stride):
        index = lax.broadcasted_iota(jnp.int32, (steps, HD), 0).astype(jnp.float32)
        angles = index * stride * freq
        return jnp.cos(angles), jnp.sin(angles)

    fine_c, fine_s = fan(STEP, 1.0)
    coarse_c, coarse_s = fan(rows // STEP, float(STEP))
    block_c, block_s = fan(SPAN + 1, float(rows))
    for i in range(rows // STEP):
        at = slice(i * STEP, (i + 1) * STEP)
        c, s = coarse_c[i : i + 1], coarse_s[i : i + 1]
        ctab[0, at, :] = fine_c * c - fine_s * s
        stab[0, at, :] = fine_s * c + fine_c * s
    base_c, base_s = ctab[0], stab[0]
    for d in range(1, SPAN + 1):
        c, s = block_c[d : d + 1], block_s[d : d + 1]
        ctab[d] = base_c * c + base_s * s
        stab[d] = (base_s * c - base_c * s) * sign
    stab[0] = base_s * sign

    scale = HD ** (-0.5) * LOG2E

    for one in q_loads:
        one.wait()

    def turn(head, carry):
        x = qraw[:, columns(head)].astype(jnp.float32)
        turned = x * (ctab[0] * scale) + pltpu.roll(x, HALF, 1) * (stab[0] * scale)
        qa[head] = turned.astype(jnp.bfloat16)
        return carry

    lax.fori_loop(0, heads, turn, 0, unroll=4)

    def seg_row(slot):
        return segs[slot].astype(jnp.float32)

    mine = seg_row(0)
    lead = mine[:, :1]
    row_at = lax.broadcasted_iota(jnp.int32, (HD, rows), 0)
    lane_at = lax.broadcasted_iota(jnp.int32, (rows, HD), 1)
    column = jnp.broadcast_to(mine, (HD, rows)).T[:, :1]
    barred = jnp.where(column == lead, 0.0, -BIG)
    ones_lane = jnp.where((lane_at >= 1) & (lane_at <= SPAN), 1.0, 0.0)
    qext[...] = jnp.where(lane_at == 0, barred, ones_lane).astype(jnp.bfloat16)
    key_at = lax.broadcasted_iota(jnp.int32, (rows, rows), 0)
    query_at = lax.broadcasted_iota(jnp.int32, (rows, rows), 1)
    mask[...] = jnp.where((key_at <= query_at) & (column == mine), 0.0, -BIG)

    for kv in range(kv_heads):
        vt[kv, HD:, :] = jnp.ones((ONES_ROWS, vt.shape[2]), jnp.bfloat16)

    def key_masks(slots):
        flat = jnp.where(row_at == 0, 1.0, 0.0)
        for slot in slots:
            bias = jnp.where(seg_row(slot) == lead, 0.0, -BIG)
            flat = jnp.where(row_at == slot, bias, flat)
        turned = flat.T
        for slot in slots:
            keep = (lane_at == 0) | (lane_at == slot)
            kext[slot] = jnp.where(keep, turned, 0.0).astype(jnp.bfloat16)

    def prepare(slots, kv):
        for slot in slots:
            x = kraw[slot, :, columns(kv)].astype(jnp.float32)
            turned = x * ctab[slot] + pltpu.roll(x, HALF, 1) * stab[slot]
            krot[kv, slot] = turned.astype(jnp.bfloat16)
            flipped = vraw[slot, :, columns(kv)].astype(jnp.float32).T
            vt[kv, :HD, slot * rows : (slot + 1) * rows] = flipped.astype(jnp.bfloat16)

    def attend(slots, kv, first, last):
        tops = {}

        def score(head, buffer):
            query = qa[head]
            if not first:
                query = jnp.concatenate([query, qext[...]], axis=1)
            best = None
            for i, slot in enumerate(slots):
                key = krot[kv, slot]
                if not first:
                    key = jnp.concatenate([key, kext[slot]], axis=1)
                part = lax.dot_general(
                    key, query, (((1,), (1,)), ((), ())), preferred_element_type=jnp.float32
                )
                if first:
                    part = part + mask[...]
                buffer[i * rows : (i + 1) * rows, :] = part
                high = jnp.max(part.reshape(rows // 8, 8, rows), axis=0)
                best = high if best is None else jnp.maximum(best, high)
            return jnp.max(best, axis=0, keepdims=True)

        def weigh(head, buffer, new_top):
            if not first:
                old_top = top[head]
                new_top = jnp.maximum(new_top, old_top)
            mixed = None
            for i, slot in enumerate(slots):
                part = buffer[i * rows : (i + 1) * rows, :]
                weights = jnp.exp2(part - new_top).astype(jnp.bfloat16)
                at = slice(slot * rows, (slot + 1) * rows)
                term = jnp.dot(vt[kv, :, at], weights, preferred_element_type=jnp.float32)
                mixed = term if mixed is None else mixed + term
            if not first:
                mixed = mixed + acc[head] * jnp.exp2(old_top - new_top)
            if last:
                result = mixed[:HD] * (1.0 / mixed[HD : HD + 1])
                out_ref[:, columns(head)] = result.T.astype(jnp.bfloat16)
            else:
                top[head] = new_top
                acc[head] = mixed

        buffers = (scores_a, scores_b)
        tops[0] = score(kv * group, buffers[0])
        for i in range(group):
            if i + 1 < group:
                tops[i + 1] = score(kv * group + i + 1, buffers[(i + 1) % 2])
            weigh(kv * group + i, buffers[i % 2], tops[i])

    near_slots = (1, 2, 3, 4)
    far_slots = (5, 6, 7)

    def own_phase(kv, carry):
        prepare((0,), kv)
        attend((0,), kv, True, False)
        return carry

    lax.fori_loop(0, kv_heads, own_phase, 0)

    relay_segs(has_behind, 4, (3, 4, 5))
    relay(has_behind, 4, (3, 4, 5), 0)
    relay_segs(has_two, 2, (6, 10))
    arrive_segs(me >= 1, 1)
    arrive_segs(me >= 3, 3)
    key_masks(near_slots)

    def near_phase(kv, carry):
        @pl.when(kv + 1 < kv_heads)
        def _():
            relay(has_behind, 4, (3, 4, 5), kv + 1)

        relay(has_two, 2, (6, 10), kv)
        for half in range(2):
            arrive(me >= 1, 1, half, kv)
            arrive(me >= 3, 3, half, kv)
        prepare(near_slots, kv)
        attend(near_slots, kv, False, False)
        return carry

    lax.fori_loop(0, kv_heads, near_phase, 0)

    relay_segs(has_eight, 8, (7, 8))
    relay(has_eight, 8, (7, 8), 0)
    relay_segs(has_six, 6, (9,))
    arrive_segs(me >= 5, 5)
    arrive_segs(me >= 7, 7)
    key_masks(far_slots)

    earlier = jnp.zeros((1, 1), jnp.float32)
    for distance in range(1, SPAN + 1):
        same = jnp.where(seg_row(distance) == lead, 1.0, 0.0)
        earlier = earlier + jnp.sum(same, axis=1, keepdims=True)
    before = jnp.sum(jnp.where(mine < column, 1.0, 0.0), axis=1, keepdims=True)
    index = lax.broadcasted_iota(jnp.int32, (rows, 1), 0).astype(jnp.float32)
    positions = index - before + jnp.where(column == lead, earlier, 0.0)
    angles = positions * freq
    cosine = jnp.cos(angles)
    sine = jnp.sin(angles) * sign
    for kv in range(kv_heads):
        at = slice(kv * HD, (kv + 1) * HD)
        x = kraw[0, :, at].astype(jnp.float32)
        rot_ref[:, at] = (x * cosine + pltpu.roll(x, HALF, 1) * sine).astype(jnp.bfloat16)

    def far_phase(kv, carry):
        @pl.when(kv + 1 < kv_heads)
        def _():
            relay(has_eight, 8, (7, 8), kv + 1)

        relay(has_six, 6, (9,), kv)
        for half in range(2):
            arrive(me >= 5, 5, half, kv)
            arrive(me >= 7, 7, half, kv)
        prepare(far_slots, kv)
        attend(far_slots, kv, False, True)
        return carry

    lax.fori_loop(0, kv_heads, far_phase, 0)

    for kind, (condition, source, distance, device) in flows.items():

        @pl.when(condition)
        def _():
            seg_copy(kind, source, distance, device).wait_send()

            def drain(kv, carry):
                for half in range(2):
                    piece_copy(kind, half, kv, source, distance, device).wait_send()
                return carry

            lax.fori_loop(0, kv_heads, drain, 0)


def local(queries, keys, values, segment_ids):
    rows = queries.shape[0]
    heads = queries.shape[1] // HD
    kv_heads = keys.shape[1] // HD
    count = lax.axis_size("seq")
    exponents = np.arange(HALF, dtype=np.float32) * np.float32(2.0 / HD)
    inverse = np.power(np.float32(ROPE_BASE), -exponents).astype(np.float32)
    frequencies = jnp.asarray(np.concatenate([inverse, inverse])[None])
    vmem = pl.BlockSpec(memory_space=pltpu.VMEM)
    hbm = pl.BlockSpec(memory_space=pltpu.HBM)
    flows = 11
    return pl.pallas_call(
        partial(kernel, kv_heads, count),
        out_shape=(
            pltpu.VMEM(queries.shape, jnp.bfloat16),
            pltpu.VMEM(keys.shape, jnp.bfloat16),
        ),
        in_specs=[hbm] * 4 + [vmem],
        out_specs=(vmem, vmem),
        scratch_shapes=[
            pltpu.VMEM((SLOTS, rows, kv_heads * HD), jnp.bfloat16),
            pltpu.VMEM((SLOTS, rows, kv_heads * HD), jnp.bfloat16),
            pltpu.VMEM((SLOTS, 1, rows), jnp.int32),
            pltpu.VMEM(queries.shape, jnp.bfloat16),
            pltpu.VMEM((heads, rows, HD), jnp.bfloat16),
            pltpu.VMEM((rows, HD), jnp.bfloat16),
            pltpu.VMEM((kv_heads, SPAN + 1, rows, HD), jnp.bfloat16),
            pltpu.VMEM((SPAN + 1, rows, HD), jnp.bfloat16),
            pltpu.VMEM((kv_heads, HD + ONES_ROWS, (SPAN + 1) * rows), jnp.bfloat16),
            pltpu.VMEM((SPAN + 1, rows, HD), jnp.float32),
            pltpu.VMEM((SPAN + 1, rows, HD), jnp.float32),
            pltpu.VMEM((rows, rows), jnp.float32),
            pltpu.VMEM((4 * rows, rows), jnp.float32),
            pltpu.VMEM((4 * rows, rows), jnp.float32),
            pltpu.VMEM((heads, 1, rows), jnp.float32),
            pltpu.VMEM((heads, HD + ONES_ROWS, rows), jnp.float32),
            pltpu.SemaphoreType.DMA((1 + 3 * kv_heads,)),
            pltpu.SemaphoreType.DMA((flows, kv_heads, 2)),
            pltpu.SemaphoreType.DMA((SLOTS, kv_heads, 2)),
            pltpu.SemaphoreType.DMA((flows,)),
            pltpu.SemaphoreType.DMA((SLOTS,)),
        ],
        compiler_params=pltpu.CompilerParams(
            vmem_limit_bytes=44 * 1024 * 1024, collective_id=0, has_side_effects=True
        ),
    )(queries, keys, values, segment_ids.reshape(1, rows), frequencies)


def solution(mesh):
    in_specs = (
        P(("groups", "seq"), None),
        P(("groups", "seq"), None),
        P(("groups", "seq"), None),
        P(("groups", "seq")),
    )
    out_specs = (P(("groups", "seq"), None), P(("groups", "seq"), None))
    return jax.shard_map(local, mesh=mesh, in_specs=in_specs, out_specs=out_specs, check_vma=False)
```

```python
from functools import partial

import jax
import jax.numpy as jnp
import numpy as np
from jax import lax
from jax.experimental import pallas as pl
from jax.experimental.pallas import tpu as pltpu
from jax.sharding import PartitionSpec as P

HD = 128
HALF = HD // 2
SPAN = 7
ROPE_BASE = 1000000.0
BIG = 1e30
NO_SEGMENT = -1
ONES_ROWS = 16
STEP = 16
SLOTS = SPAN + 2
LOG2E = 1.4426950408889634


def kernel(
    kv_heads, count, q_hbm, k_hbm, v_hbm, seg_hbm, freq_ref, out_ref, rot_ref,
    kraw, vraw, segs, qraw, qa, qext, krot, kext, vt_a, vt_b, ctab, stab, mask,
    scores_a, scores_b, weights_a, weights_b, top, fade, acc,
    local_sems, send_sems, recv_sems, seg_send, seg_recv,
):
    rows = kraw.shape[1]
    heads = qa.shape[0]
    group = heads // kv_heads
    me = lax.axis_index("seq")
    core = lax.rem(me, 2)
    side = lax.rem(me // 2, 2)
    plane = me // 4
    planes = count // 4
    partner = me + 1 - 2 * core
    across = me + 2 - 4 * side
    ahead = me + 4
    behind = me - 4
    has_ahead = plane + 1 < planes
    has_behind = plane >= 1

    barrier = pltpu.get_barrier_semaphore()

    def greet(device):
        pl.semaphore_signal(
            barrier, inc=1, device_id={"seq": device}, device_id_type=pl.DeviceIdType.MESH
        )

    greet(partner)
    greet(across)

    @pl.when(has_ahead)
    def _():
        greet(ahead)

    @pl.when(has_behind)
    def _():
        greet(behind)

    def columns(kv):
        return pl.ds(pl.multiple_of(kv * HD, HD), HD)

    def load(index, src, dst):
        return pltpu.make_async_copy(src, dst, local_sems.at[index])

    seg_load = load(0, seg_hbm, segs.at[0])
    seg_load.start()
    loads = []
    for kv in range(kv_heads):
        at = slice(kv * HD, (kv + 1) * HD)
        loads.append((
            load(1 + 2 * kv, k_hbm.at[:, at], kraw.at[0, :, at]),
            load(2 + 2 * kv, v_hbm.at[:, at], vraw.at[0, :, at]),
        ))
        for one in loads[-1]:
            one.start()
    wide = group * HD
    q_loads = []
    for kv in range(kv_heads):
        at = slice(kv * wide, (kv + 1) * wide)
        q_loads.append(load(1 + 2 * kv_heads + kv, q_hbm.at[:, at], qraw.at[:, at]))
        q_loads[-1].start()

    both = has_ahead & has_behind
    one_side = (has_ahead | has_behind) & jnp.logical_not(both)
    neither = jnp.logical_not(has_ahead | has_behind)
    for extra, condition in ((2, both), (1, one_side), (0, neither)):

        @pl.when(condition)
        def _():
            pl.semaphore_wait(barrier, 2 + extra)

    def piece_copy(kind, half, kv, source, distance, device):
        buffer = (kraw, vraw)[half]
        return pltpu.make_async_remote_copy(
            src_ref=buffer.at[source, :, columns(kv)],
            dst_ref=buffer.at[distance, :, columns(kv)],
            send_sem=send_sems.at[kind, kv, half],
            recv_sem=recv_sems.at[distance, kv, half],
            device_id={"seq": device},
            device_id_type=pl.DeviceIdType.MESH,
        )

    def seg_copy(kind, source, distance, device):
        return pltpu.make_async_remote_copy(
            src_ref=segs.at[source],
            dst_ref=segs.at[distance],
            send_sem=seg_send.at[kind],
            recv_sem=seg_recv.at[distance],
            device_id={"seq": device},
            device_id_type=pl.DeviceIdType.MESH,
        )

    to_partner = 1 - 2 * core
    relays = core == 1
    has_two = (side == 1) | has_behind
    has_six = ((side == 1) & has_behind) | (plane >= 2)
    has_eight = (plane >= 2) & relays
    flows = {
        0: (has_ahead, 0, 4, ahead),
        1: (side == 0, 0, 2, across),
        2: (core == 0, 0, 1, partner),
        3: (has_behind, 4, 6 - 4 * side, across),
        4: (has_behind & has_ahead & relays, 4, 8, ahead),
        5: (has_behind, 4, 4 + to_partner, partner),
        6: (has_two, 2, 2 + to_partner, partner),
        7: (has_eight & (side == 1), 8, 6, across),
        8: (has_eight, 8, 7, partner),
        9: (has_six, 6, 6 + to_partner, partner),
        10: ((side == 0) & (core == 0) & has_behind & has_ahead, 2, 6, ahead),
    }

    def send(kinds, half, kv):
        for kind in kinds:
            condition, source, distance, device = flows[kind]

            @pl.when(condition)
            def _():
                piece_copy(kind, half, kv, source, distance, device).start()

    def send_segs(kinds):
        for kind in kinds:
            condition, source, distance, device = flows[kind]

            @pl.when(condition)
            def _():
                seg_copy(kind, source, distance, device).start()

    def arrive(condition, distance, half, kv):
        @pl.when(condition)
        def _():
            piece_copy(0, half, kv, 0, distance, partner).wait_recv()

    def arrive_segs(condition, distance):
        @pl.when(condition)
        def _():
            seg_copy(0, 0, distance, partner).wait_recv()

    def relay(condition, distance, kinds, kv):
        for half in range(2):
            arrive(condition, distance, half, kv)
            send(kinds, half, kv)

    def relay_segs(condition, distance, kinds):
        arrive_segs(condition, distance)
        send_segs(kinds)

    seg_load.wait()
    send_segs((0, 1, 2))
    for kv in range(kv_heads):
        for half in range(2):
            loads[kv][half].wait()
            send((0, 1, 2), half, kv)

    for distance in range(1, SPAN + 1):

        @pl.when(me < distance)
        def _():
            segs[distance] = jnp.full(segs.shape[1:], NO_SEGMENT, jnp.int32)
            kraw[distance] = jnp.zeros(kraw.shape[1:], jnp.bfloat16)
            vraw[distance] = jnp.zeros(vraw.shape[1:], jnp.bfloat16)

    freq = freq_ref[...]
    lane = lax.broadcasted_iota(jnp.int32, (1, HD), 1)
    sign = jnp.where(lane < HALF, -1.0, 1.0)

    def fan(steps, stride):
        index = lax.broadcasted_iota(jnp.int32, (steps, HD), 0).astype(jnp.float32)
        angles = index * stride * freq
        return jnp.cos(angles), jnp.sin(angles)

    fine_c, fine_s = fan(STEP, 1.0)
    coarse_c, coarse_s = fan(rows // STEP, float(STEP))
    block_c, block_s = fan(SPAN + 1, float(rows))
    for i in range(rows // STEP):
        at = slice(i * STEP, (i + 1) * STEP)
        c, s = coarse_c[i : i + 1], coarse_s[i : i + 1]
        ctab[0, at, :] = fine_c * c - fine_s * s
        stab[0, at, :] = fine_s * c + fine_c * s
    base_c, base_s = ctab[0], stab[0]
    for d in range(1, SPAN + 1):
        c, s = block_c[d : d + 1], block_s[d : d + 1]
        ctab[d] = base_c * c + base_s * s
        stab[d] = (base_s * c - base_c * s) * sign
    stab[0] = base_s * sign

    scale = HD ** (-0.5) * LOG2E

    for one in q_loads:
        one.wait()

    turn_c = (ctab[0] * scale).T[:HALF]
    turn_s = (base_s * scale).T[:HALF]

    def turn(head, carry):
        x = qraw[:, columns(head)].astype(jnp.float32).T
        low, high = x[:HALF], x[HALF:]
        qa[head, :HALF, :] = (low * turn_c - high * turn_s).astype(jnp.bfloat16)
        qa[head, HALF:, :] = (high * turn_c + low * turn_s).astype(jnp.bfloat16)
        return carry

    lax.fori_loop(0, heads, turn, 0, unroll=4)

    def seg_row(slot):
        return segs[slot].astype(jnp.float32)

    mine = seg_row(0)
    lead = mine[:, :1]
    row_at = lax.broadcasted_iota(jnp.int32, (HD, rows), 0)
    lane_at = lax.broadcasted_iota(jnp.int32, (rows, HD), 1)
    column = jnp.broadcast_to(mine, (HD, rows)).T[:, :1]
    barred = jnp.where(mine == lead, 0.0, -BIG)
    ones_row = jnp.where((row_at >= 1) & (row_at <= SPAN), 1.0, 0.0)
    qext[...] = jnp.where(row_at == 0, barred, ones_row).astype(jnp.bfloat16)
    key_at = lax.broadcasted_iota(jnp.int32, (rows, rows), 0)
    query_at = lax.broadcasted_iota(jnp.int32, (rows, rows), 1)
    mask[...] = jnp.where((key_at <= query_at) & (column == mine), 0.0, -BIG)

    for vt in (vt_a, vt_b):
        vt[:, HD:, :] = jnp.ones((vt.shape[0], ONES_ROWS, rows), jnp.bfloat16)

    def key_masks(slots):
        flat = jnp.where(row_at == 0, 1.0, 0.0)
        for slot in slots:
            bias = jnp.where(seg_row(slot) == lead, 0.0, -BIG)
            flat = jnp.where(row_at == slot, bias, flat)
        turned = flat.T
        for slot in slots:
            keep = (lane_at == 0) | (lane_at == slot)
            kext[slot] = jnp.where(keep, turned, 0.0).astype(jnp.bfloat16)

    scores, weights, flipped = (scores_a, scores_b), (weights_a, weights_b), (vt_a, vt_b)
    group_at = range(group)

    def turn_keys(unit):
        slots, kv, _, _ = unit
        for i, slot in enumerate(slots):
            x = kraw[slot, :, columns(kv)].astype(jnp.float32)
            turned = x * ctab[slot] + pltpu.roll(x, HALF, 1) * stab[slot]
            krot[i] = turned.astype(jnp.bfloat16)

    def flip_values(unit, vt):
        slots, kv, _, _ = unit
        for i, slot in enumerate(slots):
            turned = vraw[slot, :, columns(kv)].astype(jnp.float32).T
            vt[i, :HD, :] = turned.astype(jnp.bfloat16)

    def score(unit, buffer):
        slots, kv, first, _ = unit
        for t in group_at:
            head = kv * group + t
            best = None
            for i, slot in enumerate(slots):
                key, query = krot[i], qa[head]
                if not first:
                    key = jnp.concatenate([key, kext[slot]], axis=1)
                    query = jnp.concatenate([query, qext[...]], axis=0)
                part = jnp.dot(key, query, preferred_element_type=jnp.float32)
                if first:
                    part = part + mask[...]
                buffer[t, i * rows : (i + 1) * rows, :] = part
                high = jnp.max(part.reshape(rows // 8, 8, rows), axis=0)
                best = high if best is None else jnp.maximum(best, high)
                if i + 1 == len(slots):
                    new_top = jnp.max(best, axis=0, keepdims=True)
                    if not first:
                        old_top = top[head]
                        new_top = jnp.maximum(old_top, new_top)
                        fade[head] = jnp.exp2(old_top - new_top)
                    top[head] = new_top
                yield

    def weigh(unit, source, target):
        slots, kv, _, _ = unit
        for t in group_at:
            height = top[kv * group + t]
            for i in range(len(slots)):
                at = slice(i * rows, (i + 1) * rows)
                target[t, at, :] = jnp.exp2(source[t, at, :] - height).astype(jnp.bfloat16)
                yield

    def mix(unit, source, vt):
        slots, kv, first, last = unit
        for t in group_at:
            head = kv * group + t
            mixed = None
            for i in range(len(slots)):
                part = source[t, i * rows : (i + 1) * rows, :]
                term = jnp.dot(vt[i], part, preferred_element_type=jnp.float32)
                mixed = term if mixed is None else mixed + term
                if i + 1 == len(slots):
                    if not first:
                        mixed = mixed + acc[head] * fade[head]
                    if last:
                        result = mixed[:HD] * (1.0 / mixed[HD : HD + 1])
                        out_ref[:, columns(head)] = result.T.astype(jnp.bfloat16)
                    else:
                        acc[head] = mixed
                yield

    def step(parity, newest, middle, oldest):
        streams = []
        if newest is not None:
            turn_keys(newest)
            streams.append((score(newest, scores[parity]), len(newest[0])))
        if middle is not None:
            flip_values(middle, flipped[1 - parity])
            streams.append((weigh(middle, scores[1 - parity], weights[1 - parity]), len(middle[0])))
        if oldest is not None:
            streams.append((mix(oldest, weights[parity], flipped[parity]), len(oldest[0])))
        beats = [
            ((k + 0.5) / (group * n), place, stream)
            for place, (stream, n) in enumerate(streams)
            for k in range(group * n)
        ]
        for _, _, stream in sorted(beats, key=lambda beat: beat[:2]):
            next(stream)

    far_slots = (5 - 4 * core, 6, 7)

    def own(kv):
        return ((0,), kv, True, False)

    def pair(index):
        base = 3 + core - 2 * (index // kv_heads)
        return ((base, base + 1), index % kv_heads, False, False)

    def rest(kv):
        return (far_slots, kv, False, True)

    def get_four(kv):
        relay(has_behind, 4, (3, 4, 5), kv)

    def get_two(kv):
        relay(has_two, 2, (6, 10), kv)

    def get_eight(kv):
        relay(has_eight, 8, (7, 8), kv)

    def get_six(kv):
        relay(has_six, 6, (9,), kv)

    def get_beside(condition, distance, kv):
        for half in range(2):
            arrive(condition, distance, half, kv)

    def get_beside_four(kv):
        get_beside(has_behind, 3 + 2 * core, kv)

    def get_beside_two(kv):
        get_beside(has_two, 1 + 2 * core, kv)

    def get_far(kv):
        get_beside(has_six, 5 + 2 * core, kv)
        get_beside((plane >= 2) & (core == 0), 7, kv)
        get_beside(core == 1, 1, kv)

    step(0, own(0), None, None)
    step(1, own(1), own(0), None)
    step(0, own(2), own(1), own(0))
    step(1, own(3), own(2), own(1))

    relay_segs(has_behind, 4, (3, 4, 5))
    get_four(0)
    arrive_segs(has_behind, 3 + 2 * core)
    key_masks((3 + core, 4 + core))
    get_beside_four(0)
    step(0, pair(0), own(3), own(2))
    get_four(1)
    get_beside_four(1)
    step(1, pair(1), pair(0), own(3))

    relay_segs(has_two, 2, (6, 10))
    arrive_segs(has_two, 1 + 2 * core)
    key_masks((1 + core, 2 + core))

    def ready(index):
        @pl.when(index < kv_heads)
        def _():
            get_four(index)

        @pl.when(index < kv_heads + 2)
        def _():
            get_two(index - 2)

        @pl.when(index < kv_heads)
        def _():
            get_beside_four(index)

        @pl.when(index >= kv_heads)
        def _():
            get_beside_two(index - kv_heads)

        @pl.when(index >= kv_heads + 2)
        def _():
            get_eight(index - kv_heads - 2)

    def pairs(turn, carry):
        index = 2 * turn + 2
        ready(index)
        step(0, pair(index), pair(index - 1), pair(index - 2))
        ready(index + 1)
        step(1, pair(index + 1), pair(index), pair(index - 1))
        return carry

    lax.fori_loop(0, kv_heads - 1, pairs, 0)
    final = 2 * kv_heads

    relay_segs(has_eight, 8, (7, 8))
    get_eight(2)
    relay_segs(has_six, 6, (9,))
    get_six(0)
    arrive_segs(has_six, 5 + 2 * core)
    arrive_segs((plane >= 2) & (core == 0), 7)
    arrive_segs(core == 1, 1)
    key_masks(far_slots)

    earlier = jnp.zeros((1, 1), jnp.float32)
    for distance in range(1, SPAN + 1):
        same = jnp.where(seg_row(distance) == lead, 1.0, 0.0)
        earlier = earlier + jnp.sum(same, axis=1, keepdims=True)
    before = jnp.sum(jnp.where(mine < column, 1.0, 0.0), axis=1, keepdims=True)
    index = lax.broadcasted_iota(jnp.int32, (rows, 1), 0).astype(jnp.float32)
    positions = index - before + jnp.where(column == lead, earlier, 0.0)
    angles = positions * freq
    cosine = jnp.cos(angles)
    sine = jnp.sin(angles) * sign
    for kv in range(kv_heads):
        at = slice(kv * HD, (kv + 1) * HD)
        x = kraw[0, :, at].astype(jnp.float32)
        rot_ref[:, at] = (x * cosine + pltpu.roll(x, HALF, 1) * sine).astype(jnp.bfloat16)

    get_far(0)
    get_six(1)
    step(0, rest(0), pair(final - 1), pair(final - 2))
    get_eight(3)
    get_far(1)
    get_six(2)
    step(1, rest(1), rest(0), pair(final - 1))
    get_far(2)
    get_six(3)
    step(0, rest(2), rest(1), rest(0))
    get_far(3)
    step(1, rest(3), rest(2), rest(1))
    step(0, None, rest(3), rest(2))
    step(1, None, None, rest(3))

    for kind, (condition, source, distance, device) in flows.items():

        @pl.when(condition)
        def _():
            seg_copy(kind, source, distance, device).wait_send()

            def drain(kv, carry):
                for half in range(2):
                    piece_copy(kind, half, kv, source, distance, device).wait_send()
                return carry

            lax.fori_loop(0, kv_heads, drain, 0)


def local(queries, keys, values, segment_ids):
    rows = queries.shape[0]
    heads = queries.shape[1] // HD
    kv_heads = keys.shape[1] // HD
    count = lax.axis_size("seq")
    exponents = np.arange(HALF, dtype=np.float32) * np.float32(2.0 / HD)
    inverse = np.power(np.float32(ROPE_BASE), -exponents).astype(np.float32)
    frequencies = jnp.asarray(np.concatenate([inverse, inverse])[None])
    vmem = pl.BlockSpec(memory_space=pltpu.VMEM)
    hbm = pl.BlockSpec(memory_space=pltpu.HBM)
    flows = 11
    return pl.pallas_call(
        partial(kernel, kv_heads, count),
        out_shape=(
            pltpu.VMEM(queries.shape, jnp.bfloat16),
            pltpu.VMEM(keys.shape, jnp.bfloat16),
        ),
        in_specs=[hbm] * 4 + [vmem],
        out_specs=(vmem, vmem),
        scratch_shapes=[
            pltpu.VMEM((SLOTS, rows, kv_heads * HD), jnp.bfloat16),
            pltpu.VMEM((SLOTS, rows, kv_heads * HD), jnp.bfloat16),
            pltpu.VMEM((SLOTS, 1, rows), jnp.int32),
            pltpu.VMEM(queries.shape, jnp.bfloat16),
            pltpu.VMEM((heads, HD, rows), jnp.bfloat16),
            pltpu.VMEM((HD, rows), jnp.bfloat16),
            pltpu.VMEM((3, rows, HD), jnp.bfloat16),
            pltpu.VMEM((SPAN + 1, rows, HD), jnp.bfloat16),
            pltpu.VMEM((3, HD + ONES_ROWS, rows), jnp.bfloat16),
            pltpu.VMEM((3, HD + ONES_ROWS, rows), jnp.bfloat16),
            pltpu.VMEM((SPAN + 1, rows, HD), jnp.float32),
            pltpu.VMEM((SPAN + 1, rows, HD), jnp.float32),
            pltpu.VMEM((rows, rows), jnp.float32),
            pltpu.VMEM((heads // kv_heads, 3 * rows, rows), jnp.float32),
            pltpu.VMEM((heads // kv_heads, 3 * rows, rows), jnp.float32),
            pltpu.VMEM((heads // kv_heads, 3 * rows, rows), jnp.bfloat16),
            pltpu.VMEM((heads // kv_heads, 3 * rows, rows), jnp.bfloat16),
            pltpu.VMEM((heads, 1, rows), jnp.float32),
            pltpu.VMEM((heads, 1, rows), jnp.float32),
            pltpu.VMEM((heads, HD + ONES_ROWS, rows), jnp.float32),
            pltpu.SemaphoreType.DMA((1 + 3 * kv_heads,)),
            pltpu.SemaphoreType.DMA((flows, kv_heads, 2)),
            pltpu.SemaphoreType.DMA((SLOTS, kv_heads, 2)),
            pltpu.SemaphoreType.DMA((flows,)),
            pltpu.SemaphoreType.DMA((SLOTS,)),
        ],
        compiler_params=pltpu.CompilerParams(
            vmem_limit_bytes=56 * 1024 * 1024, collective_id=0, has_side_effects=True
        ),
    )(
        *[
            pltpu.with_memory_space_constraint(x, pltpu.HBM)
            for x in (queries, keys, values, segment_ids.reshape(1, rows))
        ],
        frequencies,
    )


def solution(mesh):
    in_specs = (
        P(("groups", "seq"), None),
        P(("groups", "seq"), None),
        P(("groups", "seq"), None),
        P(("groups", "seq")),
    )
    out_specs = (P(("groups", "seq"), None), P(("groups", "seq"), None))
    return jax.shard_map(local, mesh=mesh, in_specs=in_specs, out_specs=out_specs, check_vma=False)
```

```python
from functools import partial

import jax
import jax.numpy as jnp
from jax import lax
from jax.experimental import pallas as pl
from jax.experimental.pallas import tpu as pltpu
from jax.sharding import PartitionSpec as P

HD = 128
HALF = HD // 2
SPAN = 7
BIG = 1e30
NO_SEGMENT = -1
ONES_ROWS = 16
STEP = 16
SLOTS = SPAN + 2
LOG2E = 1.4426950408889634
LOG2_BASE = 19.931568569324174


def kernel(
    kv_heads, count, q_hbm, k_hbm, v_hbm, seg_hbm, out_ref, rot_ref,
    kraw, vraw, segs, qraw, qa, qext, krot, kext, vt_a, vt_b, ctab, stab, mask,
    scores_a, scores_b, weights_a, weights_b, top, fade, acc,
    local_sems, send_sems, recv_sems, seg_send, seg_recv,
):
    rows = kraw.shape[2]
    heads = qa.shape[0]
    group = heads // kv_heads
    me = lax.axis_index("seq")
    core = lax.rem(me, 2)
    side = lax.rem(me // 2, 2)
    plane = me // 4
    planes = count // 4
    partner = me + 1 - 2 * core
    across = me + 2 - 4 * side
    ahead = me + 4
    has_ahead = plane + 1 < planes
    has_behind = plane >= 1

    barrier = pltpu.get_barrier_semaphore()

    def greet(device):
        pl.semaphore_signal(
            barrier, inc=1, device_id={"seq": device}, device_id_type=pl.DeviceIdType.MESH
        )

    for distance in range(1, SPAN + 1):

        @pl.when(me >= distance)
        def _():
            greet(me - distance)

        @pl.when(me + distance < count)
        def _():
            greet(me + distance)

    def columns(kv):
        return pl.ds(pl.multiple_of(kv * HD, HD), HD)

    def load(index, src, dst):
        return pltpu.make_async_copy(src, dst, local_sems.at[index])

    seg_load = load(0, seg_hbm, segs.at[0])
    seg_load.start()
    loads = []
    for kv in range(kv_heads):
        at = slice(kv * HD, (kv + 1) * HD)
        loads.append((
            load(1 + 2 * kv, k_hbm.at[:, at], kraw.at[0, kv]),
            load(2 + 2 * kv, v_hbm.at[:, at], vraw.at[0, kv]),
        ))
        for one in loads[-1]:
            one.start()
    wide = group * HD
    q_loads = []
    for kv in range(kv_heads):
        at = slice(kv * wide, (kv + 1) * wide)
        q_loads.append(load(1 + 2 * kv_heads + kv, q_hbm.at[:, at], qraw.at[:, at]))
        q_loads[-1].start()

    before_me = jnp.minimum(me, SPAN)
    after_me = jnp.minimum(count - 1 - me, SPAN)
    pl.semaphore_wait(barrier, before_me + after_me)

    def piece_copy(kind, half, kv, source, distance, device):
        buffer = (kraw, vraw)[half]
        return pltpu.make_async_remote_copy(
            src_ref=buffer.at[source, kv],
            dst_ref=buffer.at[distance, kv],
            send_sem=send_sems.at[kind, kv, half],
            recv_sem=recv_sems.at[distance, kv, half],
            device_id={"seq": device},
            device_id_type=pl.DeviceIdType.MESH,
        )

    def seg_copy(distance):
        return pltpu.make_async_remote_copy(
            src_ref=segs.at[0],
            dst_ref=segs.at[distance],
            send_sem=seg_send.at[distance],
            recv_sem=seg_recv.at[distance],
            device_id={"seq": me + distance},
            device_id_type=pl.DeviceIdType.MESH,
        )

    to_partner = 1 - 2 * core
    relays = core == 1
    has_two = (side == 1) | has_behind
    has_six = ((side == 1) & has_behind) | (plane >= 2)
    has_eight = (plane >= 2) & relays
    flows = {
        0: (has_ahead, 0, 4, ahead),
        1: (side == 0, 0, 2, across),
        2: (core == 0, 0, 1, partner),
        3: (has_behind, 4, 6 - 4 * side, across),
        4: (has_behind & has_ahead & relays, 4, 8, ahead),
        5: (has_behind, 4, 4 + to_partner, partner),
        6: (has_two, 2, 2 + to_partner, partner),
        7: (has_eight & (side == 1), 8, 6, across),
        8: (has_eight, 8, 7, partner),
        9: (has_six, 6, 6 + to_partner, partner),
        10: ((side == 0) & (core == 0) & has_behind & has_ahead, 2, 6, ahead),
        11: ((side == 1) & has_ahead, 2, 6, ahead),
    }

    def carries(kind, kv):
        condition = flows[kind][0]
        final = kv == kv_heads - 1
        if kind == 3 and final:
            return condition & (side == 1)
        if kind == 11 and not final:
            return None
        return condition

    def send(kinds, half, kv, allowed=True):
        for kind in kinds:
            _, source, distance, device = flows[kind]
            condition = carries(kind, kv)
            if condition is None:
                continue

            @pl.when(condition & allowed)
            def _():
                piece_copy(kind, half, kv, source, distance, device).start()

    def arrive(condition, distance, half, kv):
        @pl.when(condition)
        def _():
            piece_copy(0, half, kv, 0, distance, partner).wait_recv()

    def relay(condition, distance, kinds, kv, halves=(0, 1)):
        for half in halves:
            arrive(condition, distance, half, kv)
            send(kinds, half, kv, condition)

    seg_load.wait()
    for distance in range(1, SPAN + 1):

        @pl.when(me + distance < count)
        def _():
            seg_copy(distance).start()

    for kv in range(kv_heads):
        for half in range(2):
            loads[kv][half].wait()
            send((0, 1, 2), half, kv)

    for distance in range(1, SPAN + 1):

        @pl.when(me < distance)
        def _():
            segs[distance] = jnp.full(segs.shape[1:], NO_SEGMENT, jnp.int32)
            kraw[distance] = jnp.zeros(kraw.shape[1:], jnp.bfloat16)
            vraw[distance] = jnp.zeros(vraw.shape[1:], jnp.bfloat16)

    lane = lax.broadcasted_iota(jnp.int32, (1, HD), 1)
    pair_at = jnp.where(lane < HALF, lane, lane - HALF).astype(jnp.float32)
    freq = jnp.exp2(pair_at * (-2.0 / HD * LOG2_BASE))
    sign = jnp.where(lane < HALF, -1.0, 1.0)

    def fan(steps, stride):
        index = lax.broadcasted_iota(jnp.int32, (steps, HD), 0).astype(jnp.float32)
        angles = index * stride * freq
        return jnp.cos(angles), jnp.sin(angles)

    fine_c, fine_s = fan(STEP, 1.0)
    coarse_c, coarse_s = fan(rows // STEP, float(STEP))
    block_c, block_s = fan(SPAN + 1, float(rows))
    for i in range(rows // STEP):
        at = slice(i * STEP, (i + 1) * STEP)
        c, s = coarse_c[i : i + 1], coarse_s[i : i + 1]
        ctab[0, at, :] = fine_c * c - fine_s * s
        stab[0, at, :] = fine_s * c + fine_c * s
    base_c, base_s = ctab[0], stab[0]
    for d in range(1, SPAN + 1):
        c, s = block_c[d : d + 1], block_s[d : d + 1]
        ctab[d] = base_c * c + base_s * s
        stab[d] = (base_s * c - base_c * s) * sign
    stab[0] = base_s * sign

    scale = HD ** (-0.5) * LOG2E

    for one in q_loads:
        one.wait()

    turn_c = (ctab[0] * scale).T[:HALF]
    turn_s = (base_s * scale).T[:HALF]

    def turn(head, carry):
        x = qraw[:, columns(head)].astype(jnp.float32).T
        low, high = x[:HALF], x[HALF:]
        qa[head, :HALF, :] = (low * turn_c - high * turn_s).astype(jnp.bfloat16)
        qa[head, HALF:, :] = (high * turn_c + low * turn_s).astype(jnp.bfloat16)
        return carry

    lax.fori_loop(0, heads, turn, 0, unroll=4)

    def seg_row(slot):
        return segs[slot].astype(jnp.float32)

    mine = seg_row(0)
    lead = mine[:, :1]
    row_at = lax.broadcasted_iota(jnp.int32, (HD, rows), 0)
    lane_at = lax.broadcasted_iota(jnp.int32, (rows, HD), 1)
    column = jnp.broadcast_to(mine, (HD, rows)).T[:, :1]
    barred = jnp.where(mine == lead, 0.0, -BIG)
    ones_row = jnp.where((row_at >= 1) & (row_at <= SPAN), 1.0, 0.0)
    qext[...] = jnp.where(row_at == 0, barred, ones_row).astype(jnp.bfloat16)
    key_at = lax.broadcasted_iota(jnp.int32, (rows, rows), 0)
    query_at = lax.broadcasted_iota(jnp.int32, (rows, rows), 1)
    mask[...] = jnp.where((key_at <= query_at) & (column == mine), 0.0, -BIG)

    for vt in (vt_a, vt_b):
        vt[:, HD:, :] = jnp.ones((vt.shape[0], ONES_ROWS, rows), jnp.bfloat16)

    def key_masks(slots):
        flat = jnp.where(row_at == 0, 1.0, 0.0)
        for slot in slots:
            bias = jnp.where(seg_row(slot) == lead, 0.0, -BIG)
            flat = jnp.where(row_at == slot, bias, flat)
        turned = flat.T
        for slot in slots:
            keep = (lane_at == 0) | (lane_at == slot)
            kext[slot] = jnp.where(keep, turned, 0.0).astype(jnp.bfloat16)

    scores, weights, flipped = (scores_a, scores_b), (weights_a, weights_b), (vt_a, vt_b)
    group_at = range(group)

    def turn_keys(unit):
        slots, kv, _, _ = unit
        for i, slot in enumerate(slots):
            x = kraw[slot, kv].astype(jnp.float32)
            turned = x * ctab[slot] + pltpu.roll(x, HALF, 1) * stab[slot]
            krot[i] = turned.astype(jnp.bfloat16)

    def flip_values(unit, vt):
        slots, kv, _, _ = unit
        for i, slot in enumerate(slots):
            turned = vraw[slot, kv].astype(jnp.float32).T
            vt[i, :HD, :] = turned.astype(jnp.bfloat16)

    def score(unit, buffer):
        slots, kv, first, _ = unit
        for t in group_at:
            head = kv * group + t
            best = None
            for i, slot in enumerate(slots):
                key, query = krot[i], qa[head]
                if not first:
                    key = jnp.concatenate([key, kext[slot]], axis=1)
                    query = jnp.concatenate([query, qext[...]], axis=0)
                part = jnp.dot(key, query, preferred_element_type=jnp.float32)
                if first:
                    part = part + mask[...]
                buffer[t, i * rows : (i + 1) * rows, :] = part
                high = jnp.max(part.reshape(rows // 8, 8, rows), axis=0)
                best = high if best is None else jnp.maximum(best, high)
                if i + 1 == len(slots):
                    new_top = jnp.max(best, axis=0, keepdims=True)
                    if not first:
                        old_top = top[head]
                        new_top = jnp.maximum(old_top, new_top)
                        fade[head] = jnp.exp2(old_top - new_top)
                    top[head] = new_top
                yield

    def weigh(unit, source, target):
        slots, kv, _, _ = unit
        for t in group_at:
            height = top[kv * group + t]
            for i in range(len(slots)):
                at = slice(i * rows, (i + 1) * rows)
                target[t, at, :] = jnp.exp2(source[t, at, :] - height).astype(jnp.bfloat16)
                yield

    def mix(unit, source, vt):
        slots, kv, first, last = unit
        for t in group_at:
            head = kv * group + t
            mixed = None
            for i in range(len(slots)):
                part = source[t, i * rows : (i + 1) * rows, :]
                term = jnp.dot(vt[i], part, preferred_element_type=jnp.float32)
                mixed = term if mixed is None else mixed + term
                if i + 1 == len(slots):
                    if not first:
                        mixed = mixed + acc[head] * fade[head]
                    if last:
                        result = mixed[:HD] * (1.0 / mixed[HD : HD + 1])
                        out_ref[:, columns(head)] = result.T.astype(jnp.bfloat16)
                    else:
                        acc[head] = mixed
                yield

    def step(parity, newest, middle, oldest, closing=None):
        streams = []
        if newest is not None:
            turn_keys(newest)
            streams.append((score(newest, scores[parity]), len(newest[0]), 0.0, 1.0))
        if middle is not None:
            flip_values(middle, flipped[1 - parity])
            stream = weigh(middle, scores[1 - parity], weights[1 - parity])
            streams.append((stream, len(middle[0]), 0.0, 1.0))
        if oldest is not None:
            span = 1.0 if closing is None else 0.5
            stream = mix(oldest, weights[parity], flipped[parity])
            streams.append((stream, len(oldest[0]), 0.0, span))
        if closing is not None:
            stream = mix(closing, weights[1 - parity], flipped[1 - parity])
            streams.append((stream, len(closing[0]), 0.55, 0.6))
        beats = [
            (start + span * (k + 0.5) / (group * n), place, stream)
            for place, (stream, n, start, span) in enumerate(streams)
            for k in range(group * n)
        ]
        for _, _, stream in sorted(beats, key=lambda beat: beat[:2]):
            next(stream)

    far_slots = (5 - 4 * core, 6, 7)

    def own(kv):
        return ((0,), kv, True, False)

    def early(kv):
        return ((3 + core, 4 + core), kv, False, False)

    def later(kv):
        return ((1 + core, 2 + core), kv, False, False)

    def rest(kv):
        return (far_slots, kv, False, True)

    def get_four(kv, halves=(0, 1)):
        relay(has_behind, 4, (3, 4, 5), kv, halves)

    def get_two(kv):
        relay(has_two, 2, (6, 10, 11), kv)

    def get_eight(kv, where):
        relay(has_eight & (side == where), 8, (7, 8), kv)

    def get_six(kv):
        relay(has_six, 6, (9,), kv)

    def get_beside(condition, distance, kv):
        for half in range(2):
            arrive(condition, distance, half, kv)

    def get_beside_four(kv):
        get_beside(has_behind, 3 + 2 * core, kv)

    def get_beside_two(kv):
        get_beside(has_two, 1 + 2 * core, kv)

    def get_far(kv):
        get_beside(has_six, 5 + 2 * core, kv)
        get_beside((plane >= 2) & (core == 0), 7, kv)
        get_beside(core == 1, 1, kv)

    step(0, own(0), None, None)
    step(1, own(1), own(0), None)
    step(0, own(2), own(1), own(0))
    get_four(0, (0,))
    step(1, own(3), own(2), own(1))
    get_four(0, (1,))

    for distance in range(1, SPAN + 1):

        @pl.when(me >= distance)
        def _():
            seg_copy(distance).wait_recv()

    key_masks(range(1, SPAN + 1))
    get_beside_four(0)
    step(0, early(0), own(3), own(2))

    earlier = jnp.zeros((1, 1), jnp.float32)
    for distance in range(1, SPAN + 1):
        same = jnp.where(seg_row(distance) == lead, 1.0, 0.0)
        earlier = earlier + jnp.sum(same, axis=1, keepdims=True)
    before = jnp.sum(jnp.where(mine < column, 1.0, 0.0), axis=1, keepdims=True)
    index = lax.broadcasted_iota(jnp.int32, (rows, 1), 0).astype(jnp.float32)
    positions = index - before + jnp.where(column == lead, earlier, 0.0)
    angles = positions * freq
    cosine = jnp.cos(angles)
    sine = jnp.sin(angles) * sign
    for kv in range(kv_heads):
        at = slice(kv * HD, (kv + 1) * HD)
        x = kraw[0, kv].astype(jnp.float32)
        rot_ref[:, at] = (x * cosine + pltpu.roll(x, HALF, 1) * sine).astype(jnp.bfloat16)

    get_four(1)
    get_beside_four(1)
    step(1, early(1), early(0), own(3))
    get_four(2)
    get_two(0)
    get_beside_four(2)
    step(0, early(2), early(1), early(0))
    get_beside_two(0)
    step(1, later(0), early(2), early(1))
    get_four(3)
    get_two(1)
    get_beside_four(3)
    step(0, early(3), later(0), early(2))
    get_beside_two(1)
    get_eight(0, 1)
    step(1, later(1), early(3), later(0))
    get_two(2)
    get_eight(0, 0)
    get_eight(1, 1)
    get_beside_two(2)
    step(0, later(2), later(1), early(3))
    get_two(3)
    get_eight(1, 0)
    get_eight(2, 1)
    get_six(0)
    get_beside_two(3)
    step(1, later(3), later(2), later(1))
    get_eight(3, 1)
    get_six(1)
    get_far(0)
    step(0, rest(0), later(3), later(2))
    get_eight(2, 0)
    get_six(2)
    get_far(1)
    step(1, rest(1), rest(0), later(3))
    get_eight(3, 0)
    get_six(3)
    get_far(2)
    step(0, rest(2), rest(1), rest(0))
    get_far(3)
    step(1, rest(3), rest(2), rest(1))
    step(0, None, rest(3), rest(2), rest(3))

    for distance in range(1, SPAN + 1):

        @pl.when(me + distance < count)
        def _():
            seg_copy(distance).wait_send()

    for kind, (_, source, distance, device) in flows.items():
        for kv in range(kv_heads):
            condition = carries(kind, kv)
            if condition is None:
                continue

            @pl.when(condition)
            def _():
                for half in range(2):
                    piece_copy(kind, half, kv, source, distance, device).wait_send()


def local(queries, keys, values, segment_ids):
    rows = queries.shape[0]
    heads = queries.shape[1] // HD
    kv_heads = keys.shape[1] // HD
    count = lax.axis_size("seq")
    vmem = pl.BlockSpec(memory_space=pltpu.VMEM)
    hbm = pl.BlockSpec(memory_space=pltpu.HBM)
    flows = 12
    return pl.pallas_call(
        partial(kernel, kv_heads, count),
        out_shape=(
            pltpu.VMEM(queries.shape, jnp.bfloat16),
            pltpu.VMEM(keys.shape, jnp.bfloat16),
        ),
        in_specs=[hbm] * 4,
        out_specs=(vmem, vmem),
        scratch_shapes=[
            pltpu.VMEM((SLOTS, kv_heads, rows, HD), jnp.bfloat16),
            pltpu.VMEM((SLOTS, kv_heads, rows, HD), jnp.bfloat16),
            pltpu.VMEM((SLOTS, 1, rows), jnp.int32),
            pltpu.VMEM(queries.shape, jnp.bfloat16),
            pltpu.VMEM((heads, HD, rows), jnp.bfloat16),
            pltpu.VMEM((HD, rows), jnp.bfloat16),
            pltpu.VMEM((3, rows, HD), jnp.bfloat16),
            pltpu.VMEM((SPAN + 1, rows, HD), jnp.bfloat16),
            pltpu.VMEM((3, HD + ONES_ROWS, rows), jnp.bfloat16),
            pltpu.VMEM((3, HD + ONES_ROWS, rows), jnp.bfloat16),
            pltpu.VMEM((SPAN + 1, rows, HD), jnp.float32),
            pltpu.VMEM((SPAN + 1, rows, HD), jnp.float32),
            pltpu.VMEM((rows, rows), jnp.float32),
            pltpu.VMEM((heads // kv_heads, 3 * rows, rows), jnp.float32),
            pltpu.VMEM((heads // kv_heads, 3 * rows, rows), jnp.float32),
            pltpu.VMEM((heads // kv_heads, 3 * rows, rows), jnp.bfloat16),
            pltpu.VMEM((heads // kv_heads, 3 * rows, rows), jnp.bfloat16),
            pltpu.VMEM((heads, 1, rows), jnp.float32),
            pltpu.VMEM((heads, 1, rows), jnp.float32),
            pltpu.VMEM((heads, HD + ONES_ROWS, rows), jnp.float32),
            pltpu.SemaphoreType.DMA((1 + 3 * kv_heads,)),
            pltpu.SemaphoreType.DMA((flows, kv_heads, 2)),
            pltpu.SemaphoreType.DMA((SLOTS, kv_heads, 2)),
            pltpu.SemaphoreType.DMA((SLOTS,)),
            pltpu.SemaphoreType.DMA((SLOTS,)),
        ],
        compiler_params=pltpu.CompilerParams(
            vmem_limit_bytes=56 * 1024 * 1024, collective_id=0, has_side_effects=True
        ),
    )(
        *[
            pltpu.with_memory_space_constraint(x, pltpu.HBM)
            for x in (queries, keys, values, segment_ids.reshape(1, rows))
        ],
    )


def solution(mesh):
    in_specs = (
        P(("groups", "seq"), None),
        P(("groups", "seq"), None),
        P(("groups", "seq"), None),
        P(("groups", "seq")),
    )
    out_specs = (P(("groups", "seq"), None), P(("groups", "seq"), None))
    return jax.shard_map(local, mesh=mesh, in_specs=in_specs, out_specs=out_specs, check_vma=False)
```

```python
from functools import partial

import jax
import jax.numpy as jnp
from jax import lax
from jax.experimental import pallas as pl
from jax.experimental.pallas import tpu as pltpu
from jax.sharding import PartitionSpec as P

HD = 128
HALF = HD // 2
SPAN = 7
BIG = 1e30
NO_SEGMENT = -1
ONES_ROWS = 16
STEP = 16
SLOTS = SPAN + 2
LOG2E = 1.4426950408889634
QUARTER_TURN = 1.5707963267948966
LOG2_BASE = 19.931568569324174


def kernel(
    kv_heads, count, q_hbm, k_hbm, v_hbm, seg_hbm, out_ref, rot_ref,
    kraw, vraw, segs, qraw, qa, qext, krot, kext, vt_a, vt_b, ctab, stab, mask,
    scores_a, scores_b, weights_a, weights_b, top, fade, acc,
    local_sems, send_sems, recv_sems, seg_send, seg_recv,
):
    rows = kraw.shape[2]
    heads = qa.shape[0]
    group = heads // kv_heads
    me = lax.axis_index("seq")
    core = lax.rem(me, 2)
    side = lax.rem(me // 2, 2)
    plane = me // 4
    planes = count // 4
    partner = me + 1 - 2 * core
    across = me + 2 - 4 * side
    ahead = me + 4
    has_ahead = plane + 1 < planes
    has_behind = plane >= 1

    barrier = pltpu.get_barrier_semaphore()

    def greet(device):
        pl.semaphore_signal(
            barrier, inc=1, device_id={"seq": device}, device_id_type=pl.DeviceIdType.MESH
        )

    for distance in range(1, SPAN + 1):

        @pl.when(me >= distance)
        def _():
            greet(me - distance)

        @pl.when(me + distance < count)
        def _():
            greet(me + distance)

    def columns(kv):
        return pl.ds(pl.multiple_of(kv * HD, HD), HD)

    def load(index, src, dst):
        return pltpu.make_async_copy(src, dst, local_sems.at[index])

    seg_load = load(0, seg_hbm, segs.at[0])
    seg_load.start()
    loads = []
    for kv in range(kv_heads):
        at = slice(kv * HD, (kv + 1) * HD)
        loads.append((
            load(1 + 2 * kv, k_hbm.at[:, at], kraw.at[0, kv]),
            load(2 + 2 * kv, v_hbm.at[:, at], vraw.at[0, kv]),
        ))
        for one in loads[-1]:
            one.start()
    wide = group * HD
    q_loads = []
    for kv in range(kv_heads):
        at = slice(kv * wide, (kv + 1) * wide)
        q_loads.append(load(1 + 2 * kv_heads + kv, q_hbm.at[:, at], qraw.at[:, at]))
        q_loads[-1].start()

    before_me = jnp.minimum(me, SPAN)
    after_me = jnp.minimum(count - 1 - me, SPAN)
    pl.semaphore_wait(barrier, before_me + after_me)

    def piece_copy(kind, half, kv, source, distance, device):
        buffer = (kraw, vraw)[half]
        return pltpu.make_async_remote_copy(
            src_ref=buffer.at[source, kv],
            dst_ref=buffer.at[distance, kv],
            send_sem=send_sems.at[kind, kv, half],
            recv_sem=recv_sems.at[distance, kv, half],
            device_id={"seq": device},
            device_id_type=pl.DeviceIdType.MESH,
        )

    def seg_copy(distance):
        return pltpu.make_async_remote_copy(
            src_ref=segs.at[0],
            dst_ref=segs.at[distance],
            send_sem=seg_send.at[distance],
            recv_sem=seg_recv.at[distance],
            device_id={"seq": me + distance},
            device_id_type=pl.DeviceIdType.MESH,
        )

    to_partner = 1 - 2 * core
    relays = core == 1
    has_two = (side == 1) | has_behind
    has_six = ((side == 1) & has_behind) | (plane >= 2)
    has_eight = (plane >= 2) & relays
    flows = {
        0: (has_ahead, 0, 4, ahead),
        1: (side == 0, 0, 2, across),
        2: (core == 0, 0, 1, partner),
        3: (has_behind, 4, 6 - 4 * side, across),
        4: (has_behind & has_ahead & relays, 4, 8, ahead),
        5: (has_behind, 4, 4 + to_partner, partner),
        6: (has_two, 2, 2 + to_partner, partner),
        7: (has_eight & (side == 1), 8, 6, across),
        8: (has_eight, 8, 7, partner),
        9: (has_six, 6, 6 + to_partner, partner),
        10: ((side == 0) & (core == 0) & has_behind & has_ahead, 2, 6, ahead),
        11: ((side == 1) & has_ahead, 2, 6, ahead),
    }

    def carries(kind, kv):
        condition = flows[kind][0]
        final = kv == kv_heads - 1
        if kind == 3 and final:
            return condition & (side == 1)
        if kind == 11 and not final:
            return None
        return condition

    def send(kinds, half, kv, allowed=True):
        for kind in kinds:
            _, source, distance, device = flows[kind]
            condition = carries(kind, kv)
            if condition is None:
                continue

            @pl.when(condition & allowed)
            def _():
                piece_copy(kind, half, kv, source, distance, device).start()

    def arrive(condition, distance, half, kv):
        @pl.when(condition)
        def _():
            piece_copy(0, half, kv, 0, distance, partner).wait_recv()

    def relay(condition, distance, kinds, kv, halves=(0, 1)):
        for half in halves:
            arrive(condition, distance, half, kv)
            send(kinds, half, kv, condition)

    seg_load.wait()
    for distance in range(1, SPAN + 1):

        @pl.when(me + distance < count)
        def _():
            seg_copy(distance).start()

    for kv in range(kv_heads):
        for half in range(2):
            loads[kv][half].wait()
            send((0, 1, 2), half, kv)

    for distance in range(1, SPAN + 1):

        @pl.when(me < distance)
        def _():
            segs[distance] = jnp.full(segs.shape[1:], NO_SEGMENT, jnp.int32)
            kraw[distance] = jnp.zeros(kraw.shape[1:], jnp.bfloat16)
            vraw[distance] = jnp.zeros(vraw.shape[1:], jnp.bfloat16)

    lane = lax.broadcasted_iota(jnp.int32, (1, HD), 1)
    pair_at = jnp.where(lane < HALF, lane, lane - HALF).astype(jnp.float32)
    freq = jnp.exp2(pair_at * (-2.0 / HD * LOG2_BASE))
    sign = jnp.where(lane < HALF, -1.0, 1.0)

    def fan(steps, stride):
        index = lax.broadcasted_iota(jnp.int32, (steps, HD), 0).astype(jnp.float32)
        angles = index * stride * freq
        return jnp.cos(angles), jnp.sin(angles)

    fine_c, fine_s = fan(STEP, 1.0)
    coarse_c, coarse_s = fan(rows // STEP, float(STEP))
    block_c, block_s = fan(SPAN + 1, float(rows))
    for i in range(rows // STEP):
        at = slice(i * STEP, (i + 1) * STEP)
        c, s = coarse_c[i : i + 1], coarse_s[i : i + 1]
        ctab[0, at, :] = fine_c * c - fine_s * s
        stab[0, at, :] = fine_s * c + fine_c * s
    base_c, base_s = ctab[0], stab[0]
    for d in range(1, SPAN + 1):
        c, s = block_c[d : d + 1], block_s[d : d + 1]
        ctab[d] = base_c * c + base_s * s
        stab[d] = (base_s * c - base_c * s) * sign
    stab[0] = base_s * sign

    scale = HD ** (-0.5) * LOG2E

    for one in q_loads:
        one.wait()

    turn_c = (ctab[0] * scale).T[:HALF]
    turn_s = (base_s * scale).T[:HALF]

    def turn(head, carry):
        x = qraw[:, columns(head)].astype(jnp.float32).T
        low, high = x[:HALF], x[HALF:]
        qa[head, :HALF, :] = (low * turn_c - high * turn_s).astype(jnp.bfloat16)
        qa[head, HALF:, :] = (high * turn_c + low * turn_s).astype(jnp.bfloat16)
        return carry

    lax.fori_loop(0, heads, turn, 0, unroll=4)

    def seg_row(slot):
        return segs[slot].astype(jnp.float32)

    mine = seg_row(0)
    lead = mine[:, :1]
    row_at = lax.broadcasted_iota(jnp.int32, (HD, rows), 0)
    lane_at = lax.broadcasted_iota(jnp.int32, (rows, HD), 1)
    column = jnp.broadcast_to(mine, (HD, rows)).T[:, :1]
    barred = jnp.where(mine == lead, 0.0, -BIG)
    ones_row = jnp.where((row_at >= 1) & (row_at <= SPAN), 1.0, 0.0)
    qext[...] = jnp.where(row_at == 0, barred, ones_row).astype(jnp.bfloat16)
    key_at = lax.broadcasted_iota(jnp.int32, (rows, rows), 0)
    query_at = lax.broadcasted_iota(jnp.int32, (rows, rows), 1)
    mask[...] = jnp.where((key_at <= query_at) & (column == mine), 0.0, -BIG)

    for vt in (vt_a, vt_b):
        vt[:, HD:, :] = jnp.ones((vt.shape[0], ONES_ROWS, rows), jnp.bfloat16)

    def key_masks(slots):
        flat = jnp.where(row_at == 0, 1.0, 0.0)
        for slot in slots:
            bias = jnp.where(seg_row(slot) == lead, 0.0, -BIG)
            flat = jnp.where(row_at == slot, bias, flat)
        turned = flat.T
        for slot in slots:
            keep = (lane_at == 0) | (lane_at == slot)
            kext[slot] = jnp.where(keep, turned, 0.0).astype(jnp.bfloat16)

    scores, weights, flipped = (scores_a, scores_b), (weights_a, weights_b), (vt_a, vt_b)
    group_at = range(group)

    def turn_keys(unit):
        slots, kv, _, _ = unit
        for i, slot in enumerate(slots):
            x = kraw[slot, kv].astype(jnp.float32)
            turned = x * ctab[slot] + pltpu.roll(x, HALF, 1) * stab[slot]
            krot[i] = turned.astype(jnp.bfloat16)

    def flip_values(unit, vt):
        slots, kv, _, _ = unit
        for i, slot in enumerate(slots):
            turned = vraw[slot, kv].astype(jnp.float32).T
            vt[i, :HD, :] = turned.astype(jnp.bfloat16)

    def score(unit, buffer):
        slots, kv, first, _ = unit
        for t in group_at:
            head = kv * group + t
            best = None
            for i, slot in enumerate(slots):
                key, query = krot[i], qa[head]
                if not first:
                    key = jnp.concatenate([key, kext[slot]], axis=1)
                    query = jnp.concatenate([query, qext[...]], axis=0)
                part = jnp.dot(key, query, preferred_element_type=jnp.float32)
                if first:
                    part = part + mask[...]
                buffer[t, i * rows : (i + 1) * rows, :] = part
                high = jnp.max(part.reshape(rows // 8, 8, rows), axis=0)
                best = high if best is None else jnp.maximum(best, high)
                if i + 1 == len(slots):
                    new_top = jnp.max(best, axis=0, keepdims=True)
                    if not first:
                        old_top = top[head]
                        new_top = jnp.maximum(old_top, new_top)
                        fade[head] = jnp.exp2(old_top - new_top)
                    top[head] = new_top
                yield

    def weigh(unit, source, target):
        slots, kv, _, _ = unit
        for t in group_at:
            height = top[kv * group + t]
            for i in range(len(slots)):
                at = slice(i * rows, (i + 1) * rows)
                target[t, at, :] = jnp.exp2(source[t, at, :] - height).astype(jnp.bfloat16)
                yield

    def mix(unit, source, vt):
        slots, kv, first, last = unit
        for t in group_at:
            head = kv * group + t
            mixed = None
            for i in range(len(slots)):
                part = source[t, i * rows : (i + 1) * rows, :]
                term = jnp.dot(vt[i], part, preferred_element_type=jnp.float32)
                mixed = term if mixed is None else mixed + term
                if i + 1 == len(slots):
                    if not first:
                        mixed = mixed + acc[head] * fade[head]
                    if last:
                        result = mixed[:HD] * (1.0 / mixed[HD : HD + 1])
                        out_ref[:, columns(head)] = result.T.astype(jnp.bfloat16)
                    else:
                        acc[head] = mixed
                yield

    def step(parity, newest, middle, oldest, closing=None):
        streams = []
        if newest is not None:
            turn_keys(newest)
            streams.append((score(newest, scores[parity]), len(newest[0]), 0.0, 1.0))
        if middle is not None:
            flip_values(middle, flipped[1 - parity])
            stream = weigh(middle, scores[1 - parity], weights[1 - parity])
            streams.append((stream, len(middle[0]), 0.0, 1.0))
        if oldest is not None:
            span = 1.0 if closing is None else 0.5
            stream = mix(oldest, weights[parity], flipped[parity])
            streams.append((stream, len(oldest[0]), 0.0, span))
        if closing is not None:
            stream = mix(closing, weights[1 - parity], flipped[1 - parity])
            streams.append((stream, len(closing[0]), 0.55, 0.6))
        beats = [
            (start + span * (k + 0.5) / (group * n), place, stream)
            for place, (stream, n, start, span) in enumerate(streams)
            for k in range(group * n)
        ]
        for _, _, stream in sorted(beats, key=lambda beat: beat[:2]):
            next(stream)

    far_slots = (5 - 4 * core, 6, 7)

    def own(kv):
        return ((0,), kv, True, False)

    def early(kv):
        return ((3 + core, 4 + core), kv, False, False)

    def later(kv):
        return ((1 + core, 2 + core), kv, False, False)

    def rest(kv):
        return (far_slots, kv, False, True)

    def get_four(kv, halves=(0, 1)):
        relay(has_behind, 4, (3, 4, 5), kv, halves)

    def get_two(kv):
        relay(has_two, 2, (6, 10, 11), kv)

    def get_eight(kv, where):
        relay(has_eight & (side == where), 8, (7, 8), kv)

    def get_six(kv):
        relay(has_six, 6, (9,), kv)

    def get_beside(condition, distance, kv):
        for half in range(2):
            arrive(condition, distance, half, kv)

    def get_beside_four(kv):
        get_beside(has_behind, 3 + 2 * core, kv)

    def get_beside_two(kv):
        get_beside(has_two, 1 + 2 * core, kv)

    def get_far(kv):
        get_beside(has_six, 5 + 2 * core, kv)
        get_beside((plane >= 2) & (core == 0), 7, kv)
        get_beside(core == 1, 1, kv)

    step(0, own(0), None, None)
    step(1, own(1), own(0), None)
    step(0, own(2), own(1), own(0))
    get_four(0, (0,))
    step(1, own(3), own(2), own(1))
    get_four(0, (1,))

    for distance in range(1, SPAN + 1):

        @pl.when(me >= distance)
        def _():
            seg_copy(distance).wait_recv()

    key_masks(range(1, SPAN + 1))
    get_beside_four(0)
    step(0, early(0), own(3), own(2))

    earlier = jnp.zeros((1, 1), jnp.float32)
    for distance in range(1, SPAN + 1):
        same = jnp.where(seg_row(distance) == lead, 1.0, 0.0)
        earlier = earlier + jnp.sum(same, axis=1, keepdims=True)
    before = jnp.sum(jnp.where(mine < column, 1.0, 0.0), axis=1, keepdims=True)
    index = lax.broadcasted_iota(jnp.int32, (rows, 1), 0).astype(jnp.float32)
    positions = index - before + jnp.where(column == lead, earlier, 0.0)
    angles = positions * freq
    both = jnp.cos(angles - jnp.where(lane < HALF, 0.0, QUARTER_TURN))
    swapped = pltpu.roll(both, HALF, 1)
    cosine = jnp.where(lane < HALF, both, swapped)
    sine = jnp.where(lane < HALF, swapped, both) * sign
    for kv in range(kv_heads):
        at = slice(kv * HD, (kv + 1) * HD)
        x = kraw[0, kv].astype(jnp.float32)
        rot_ref[:, at] = (x * cosine + pltpu.roll(x, HALF, 1) * sine).astype(jnp.bfloat16)

    get_four(1)
    get_beside_four(1)
    step(1, early(1), early(0), own(3))
    get_four(2)
    get_two(0)
    get_beside_four(2)
    step(0, early(2), early(1), early(0))
    get_beside_two(0)
    step(1, later(0), early(2), early(1))
    get_four(3)
    get_two(1)
    get_beside_four(3)
    step(0, early(3), later(0), early(2))
    get_beside_two(1)
    get_eight(0, 1)
    step(1, later(1), early(3), later(0))
    get_two(2)
    get_eight(0, 0)
    get_eight(1, 1)
    get_beside_two(2)
    step(0, later(2), later(1), early(3))
    get_two(3)
    get_eight(1, 0)
    get_eight(2, 1)
    get_six(0)
    get_beside_two(3)
    step(1, later(3), later(2), later(1))
    get_eight(3, 1)
    get_six(1)
    get_far(0)
    step(0, rest(0), later(3), later(2))
    get_eight(2, 0)
    get_six(2)
    get_far(1)
    step(1, rest(1), rest(0), later(3))
    get_eight(3, 0)
    get_six(3)
    get_far(2)
    step(0, rest(2), rest(1), rest(0))
    get_far(3)
    step(1, rest(3), rest(2), rest(1))
    step(0, None, rest(3), rest(2), rest(3))

    for distance in range(1, SPAN + 1):

        @pl.when(me + distance < count)
        def _():
            seg_copy(distance).wait_send()

    for kind, (_, source, distance, device) in flows.items():
        for kv in range(kv_heads):
            condition = carries(kind, kv)
            if condition is None:
                continue

            @pl.when(condition)
            def _():
                for half in range(2):
                    piece_copy(kind, half, kv, source, distance, device).wait_send()


def local(queries, keys, values, segment_ids):
    rows = queries.shape[0]
    heads = queries.shape[1] // HD
    kv_heads = keys.shape[1] // HD
    count = lax.axis_size("seq")
    vmem = pl.BlockSpec(memory_space=pltpu.VMEM)
    hbm = pl.BlockSpec(memory_space=pltpu.HBM)
    flows = 12
    return pl.pallas_call(
        partial(kernel, kv_heads, count),
        out_shape=(
            pltpu.VMEM(queries.shape, jnp.bfloat16),
            pltpu.VMEM(keys.shape, jnp.bfloat16),
        ),
        in_specs=[hbm] * 4,
        out_specs=(vmem, vmem),
        scratch_shapes=[
            pltpu.VMEM((SLOTS, kv_heads, rows, HD), jnp.bfloat16),
            pltpu.VMEM((SLOTS, kv_heads, rows, HD), jnp.bfloat16),
            pltpu.VMEM((SLOTS, 1, rows), jnp.int32),
            pltpu.VMEM(queries.shape, jnp.bfloat16),
            pltpu.VMEM((heads, HD, rows), jnp.bfloat16),
            pltpu.VMEM((HD, rows), jnp.bfloat16),
            pltpu.VMEM((3, rows, HD), jnp.bfloat16),
            pltpu.VMEM((SPAN + 1, rows, HD), jnp.bfloat16),
            pltpu.VMEM((3, HD + ONES_ROWS, rows), jnp.bfloat16),
            pltpu.VMEM((3, HD + ONES_ROWS, rows), jnp.bfloat16),
            pltpu.VMEM((SPAN + 1, rows, HD), jnp.float32),
            pltpu.VMEM((SPAN + 1, rows, HD), jnp.float32),
            pltpu.VMEM((rows, rows), jnp.float32),
            pltpu.VMEM((heads // kv_heads, 3 * rows, rows), jnp.float32),
            pltpu.VMEM((heads // kv_heads, 3 * rows, rows), jnp.float32),
            pltpu.VMEM((heads // kv_heads, 3 * rows, rows), jnp.bfloat16),
            pltpu.VMEM((heads // kv_heads, 3 * rows, rows), jnp.bfloat16),
            pltpu.VMEM((heads, 1, rows), jnp.float32),
            pltpu.VMEM((heads, 1, rows), jnp.float32),
            pltpu.VMEM((heads, HD + ONES_ROWS, rows), jnp.float32),
            pltpu.SemaphoreType.DMA((1 + 3 * kv_heads,)),
            pltpu.SemaphoreType.DMA((flows, kv_heads, 2)),
            pltpu.SemaphoreType.DMA((SLOTS, kv_heads, 2)),
            pltpu.SemaphoreType.DMA((SLOTS,)),
            pltpu.SemaphoreType.DMA((SLOTS,)),
        ],
        compiler_params=pltpu.CompilerParams(
            vmem_limit_bytes=56 * 1024 * 1024, collective_id=0, has_side_effects=True
        ),
    )(
        *[
            pltpu.with_memory_space_constraint(x, pltpu.HBM)
            for x in (queries, keys, values, segment_ids.reshape(1, rows))
        ],
    )


def solution(mesh):
    in_specs = (
        P(("groups", "seq"), None),
        P(("groups", "seq"), None),
        P(("groups", "seq"), None),
        P(("groups", "seq")),
    )
    out_specs = (P(("groups", "seq"), None), P(("groups", "seq"), None))
    return jax.shard_map(local, mesh=mesh, in_specs=in_specs, out_specs=out_specs, check_vma=False)
```
